32 devices in a mesh: patch: 16 (over z, y, core), band: 2 (over x).
Axes of the slice: x: 2, y: 2, z: 4, core: 2. Of those that a mesh axis runs over, the one named last changes fastest.
Arguments:
- latents: float32 [10240, 512], P('patch', 'band'), may hold values from -6 to 6
- edge_latents: float32 [81920, 512], P(('patch', 'band')), may hold values from -6 to 6
- edge_sender: int32 [81920], P(('patch', 'band')), may hold values from 0 to 575, as said below
- edge_receiver: int32 [81920], P(('patch', 'band')), may hold values from 0 to 319
- block_counts: int32 [640], P(('patch', 'band')), may hold values from 16 to 128, as said below
- send_rows: int32 [32, 32, 8], P(('patch', 'band')), may hold values from 0 to 319
- edge_first_weight: bfloat16 [2, 1536, 512], replicated, may hold values from -0.15625 to 0.15625
- edge_first_bias: float32 [2, 512], replicated, may hold values from -3 to 3
- edge_second_weight: bfloat16 [2, 512, 512], replicated
- edge_gain: float32 [2, 512], replicated, may hold values from 0.1 to 1.9
- edge_offset: float32 [2, 512], replicated, may hold values from -3 to 3
- node_first_weight: bfloat16 [2, 1024, 512], replicated, may hold values from -0.1875 to 0.1875
- node_first_bias: float32 [2, 512], replicated, may hold values from -3 to 3
- node_second_weight: bfloat16 [2, 512, 512], replicated
- node_gain: float32 [2, 512], replicated, may hold values from 0.1 to 1.9
- node_offset: float32 [2, 512], replicated, may hold values from -3 to 3
Outputs:
- new_nodes: float32 [10240, 512], P(('patch', 'band'))
- new_edges: float32 [81920, 512], P(('patch', 'band'))
The draws below stay inside these ranges and needn't reach their ends.
Inputs may be any that keep to these rules, and one draw needn't show every extreme that they name: `edge_sender`: an entry below 320 names a node row of the edge's own device; an entry k above names slot (k - 320) % 8 of the rows that device (k - 320) // 8 sends to the edge's device. `block_counts`: the used slots of a block are its first ones; every device has a full block. send_rows[d, q] lists node rows of device d, numbered within d, that device q receives from d.
All inputs are finite; a program needn't handle non-finite values.
Results may differ from the reference program's by a relative error of at most 0.0045.
Values may be sent and summed in bfloat16 or wider, within the bound.
A program may use at most 128 MiB of HBM per device.

```python
import math
import jax
import jax.numpy as jnp
from jax import lax

D = 512
HID = 512
NODE_DEV = 320
BLOCKS = 20
BLOCK = 128
SLOT = 8
LAYERS = 2
SHARDS = 32
NODES = 10240
EDGE_DEV = 2560
EDGES = 81920


def draw_edge_sender(key, part):
    subkeys = jax.random.split(jax.random.fold_in(key, 5), 6)
    shape_two = (SHARDS, EDGE_DEV)
    lower = SLOT // 2 + 1
    counts = lower + jax.random.randint(subkeys[0], (SHARDS, SHARDS), 0, 1 << 20) % (SLOT + 1 - lower)
    fullest = jax.random.randint(subkeys[1], (SHARDS, 1), 0, SHARDS)
    counts = jnp.where(jnp.arange(SHARDS)[None, :] == fullest, SLOT, counts)
    local_rows = jax.random.randint(subkeys[2], shape_two, 0, NODE_DEV)
    source_shard = jax.random.randint(subkeys[3], shape_two, 0, SHARDS)
    spread_bits = jax.random.randint(subkeys[4], shape_two, 0, 1 << 20)
    chosen = jnp.take_along_axis(counts, source_shard, axis=1)
    remote = NODE_DEV + source_shard * SLOT + spread_bits % chosen
    picker = jax.random.randint(subkeys[5], shape_two, 0, 2)
    return jnp.where(picker == 0, local_rows, remote).reshape(-1).astype(jnp.int32)


def draw_block_counts(key, part):
    subkeys = jax.random.split(jax.random.fold_in(key, 7), 3)
    floor_value = max(1, BLOCK // 8)
    device_low = jax.random.randint(subkeys[0], (SHARDS, 1), floor_value, BLOCK + 1)
    raw_bits = jax.random.randint(subkeys[1], (SHARDS, BLOCKS), 0, 1 << 20)
    counts = device_low + raw_bits % (BLOCK + 1 - device_low)
    full_block = jax.random.randint(subkeys[2], (SHARDS, 1), 0, BLOCKS)
    counts = jnp.where(jnp.arange(BLOCKS)[None, :] == full_block, BLOCK, counts)
    return counts.reshape(-1).astype(jnp.int32)


def scaled_weight(key, depth_count, fan_rows, fan_cols):
    subkeys = jax.random.split(key, 2)
    base = jax.random.normal(subkeys[0], (depth_count, fan_rows, fan_cols), jnp.float32)
    column_scale = jnp.exp(jax.random.uniform(subkeys[1], (depth_count, 1, fan_cols), jnp.float32, math.log(0.3), math.log(3.0)))
    return base * column_scale * fan_rows ** (-0.5)


def draw_edge_second_weight(key, part):
    return scaled_weight(jax.random.fold_in(key, 21), LAYERS, HID, D).astype(jnp.bfloat16)


def draw_node_second_weight(key, part):
    return scaled_weight(jax.random.fold_in(key, 23), LAYERS, HID, D).astype(jnp.bfloat16)


def with_ends(array, stream_key, low, top_value):
    longest = array.shape.index(max(array.shape))
    spots = []
    for shift in (0, 1):
        where = [jax.random.randint(jax.random.fold_in(stream_key, axis), (), 0, length) for axis, length in enumerate(array.shape)]
        where[longest] = (where[longest] + shift) % array.shape[longest]
        spots.append(tuple(where))
    return array.at[spots[0]].set(low).at[spots[1]].set(top_value)


def levels(own_key, shape, cuts, low, largest):
    loudness = 1.0
    for dim, parts in cuts:
        heights = jax.random.uniform(jax.random.fold_in(jax.random.fold_in(own_key, 6), dim), (parts,), jnp.float32, low / len(cuts), largest / len(cuts))
        loudness = loudness * jnp.repeat(jnp.exp(heights), shape[dim] // parts).reshape((-1,) + (1,) * (len(shape) - 1 - dim))
    return loudness


def gaussian(own_key, dims, scale, limit, cuts=(), kind=jnp.bfloat16):
    values = jax.random.normal(own_key, dims, jnp.float32) * scale
    if len(cuts) > 0:
        values = levels(own_key, dims, cuts, -0.22, 0.18) * values
    return jnp.clip(values, min=-limit, max=limit).astype(kind)


def setup_inputs(seed: int = 0) -> dict:
    arg_keys = jax.random.split(jax.random.key(seed), 17)
    latents = gaussian(arg_keys[0], (NODES, D), 1.0, 6.0, ((0, 16), (1, 2)), jnp.float32)
    edge_latents = gaussian(arg_keys[1], (EDGES, D), 1.0, 6.0, ((0, 32),), jnp.float32)
    edge_sender = draw_edge_sender(jax.random.fold_in(arg_keys[16], 71), 0)
    edge_receiver = with_ends(jax.random.randint(arg_keys[3], (EDGES,), 0, NODE_DEV), jax.random.fold_in(arg_keys[3], 1), 0, NODE_DEV - 1).astype(jnp.int32)
    block_counts = draw_block_counts(jax.random.fold_in(arg_keys[16], 71), 0)
    send_rows = with_ends(jax.random.randint(arg_keys[5], (SHARDS, SHARDS, SLOT), 0, NODE_DEV), jax.random.fold_in(arg_keys[5], 1), 0, NODE_DEV - 1).astype(jnp.int32)
    edge_first_weight = gaussian(arg_keys[6], (LAYERS, 3 * D, HID), (3 * D) ** -0.5, 0.15625)
    edge_first_bias = gaussian(arg_keys[7], (LAYERS, HID), 0.5, 3.0, (), jnp.float32)
    edge_second_weight = draw_edge_second_weight(jax.random.fold_in(arg_keys[16], 71), 0)
    edge_gain = jnp.clip(1.0 + 0.18 * jax.random.normal(arg_keys[9], (LAYERS, D), jnp.float32), 0.1, 1.9)
    edge_offset = gaussian(arg_keys[10], (LAYERS, D), 0.5, 3.0, (), jnp.float32)
    node_first_weight = gaussian(arg_keys[11], (LAYERS, 2 * D, HID), (2 * D) ** -0.5, 0.1875)
    node_first_bias = gaussian(arg_keys[12], (LAYERS, HID), 0.5, 3.0, (), jnp.float32)
    node_second_weight = draw_node_second_weight(jax.random.fold_in(arg_keys[16], 71), 0)
    node_gain = jnp.clip(1.0 + 0.18 * jax.random.normal(arg_keys[14], (LAYERS, D), jnp.float32), 0.1, 1.9)
    node_offset = gaussian(arg_keys[15], (LAYERS, D), 0.5, 3.0, (), jnp.float32)
    return {"latents": latents, "edge_latents": edge_latents, "edge_sender": edge_sender, "edge_receiver": edge_receiver, "block_counts": block_counts, "send_rows": send_rows, "edge_first_weight": edge_first_weight, "edge_first_bias": edge_first_bias, "edge_second_weight": edge_second_weight, "edge_gain": edge_gain, "edge_offset": edge_offset, "node_first_weight": node_first_weight, "node_first_bias": node_first_bias, "node_second_weight": node_second_weight, "node_gain": node_gain, "node_offset": node_offset}


epsilon = 1e-05

def layer_norm(values, norm_gain, norm_offset):
    centre = values - lax.optimization_barrier(jnp.mean(values, axis=-1, keepdims=True))
    spread = lax.optimization_barrier(jnp.mean(centre * centre, axis=-1, keepdims=True))
    return centre * lax.rsqrt(spread + epsilon) * norm_gain + norm_offset

def perceptron(pieces, first_weight, first_bias, second_weight, norm_gain, norm_offset):
    columns = pieces[0].shape[1]
    running = first_bias
    for position in range(len(pieces)):
        running = running + jnp.dot(pieces[position], first_weight[position * columns:(position + 1) * columns], preferred_element_type=jnp.float32)
    active = (running * jax.nn.sigmoid(running)).astype(jnp.bfloat16)
    result = jnp.dot(active, second_weight, preferred_element_type=jnp.float32)
    return layer_norm(result, norm_gain, norm_offset)

def reference(latents, edge_latents, edge_sender, edge_receiver, block_counts, send_rows, edge_first_weight, edge_first_bias, edge_second_weight, edge_gain, edge_offset, node_first_weight, node_first_bias, node_second_weight, node_gain, node_offset):
    shards = NODES // NODE_DEV
    slot_index = jnp.arange(EDGES, dtype=jnp.int32)
    owning = slot_index // EDGE_DEV
    beyond = edge_sender - NODE_DEV
    source_shard = jnp.clip(beyond // SLOT, 0, shards - 1).astype(jnp.int32)
    slot_pos = jnp.clip(beyond % SLOT, 0, SLOT - 1).astype(jnp.int32)
    remote = source_shard * NODE_DEV + send_rows[source_shard, owning, slot_pos]
    senders = jnp.where(edge_sender < NODE_DEV, owning * NODE_DEV + edge_sender, remote).astype(jnp.int32)
    receivers = (owning * NODE_DEV + edge_receiver).astype(jnp.int32)
    usable = slot_index % BLOCK < block_counts[slot_index // BLOCK]
    node_state = latents
    edge_state = edge_latents
    for layer_index in range(LAYERS):
        node_low = node_state.astype(jnp.bfloat16)

        def portion(operands):
            edge_part, send_part, recv_part = operands
            return perceptron((edge_part.astype(jnp.bfloat16), node_low[send_part], node_low[recv_part]), edge_first_weight[layer_index], edge_first_bias[layer_index], edge_second_weight[layer_index], edge_gain[layer_index], edge_offset[layer_index])
        update = lax.map(portion, (edge_state.reshape(shards, EDGE_DEV, D), senders.reshape(shards, EDGE_DEV), receivers.reshape(shards, EDGE_DEV)))
        update = update.reshape(EDGES, D)
        edge_state = edge_state + jnp.where(usable[:, None], update, jnp.zeros_like(update))
        edge_out_low = lax.optimization_barrier(edge_state.astype(jnp.bfloat16)).astype(jnp.float32)
        summed = jax.ops.segment_sum(jnp.where(usable[:, None], edge_out_low, jnp.zeros_like(edge_out_low)), receivers, num_segments=NODES)
        summed_low = summed.astype(jnp.bfloat16)
        node_state = node_state + perceptron((node_low, summed_low), node_first_weight[layer_index], node_first_bias[layer_index], node_second_weight[layer_index], node_gain[layer_index], node_offset[layer_index])
    return (node_state, edge_state)
```

```python
import functools

import jax
import jax.numpy as jnp
from jax import lax
from jax.experimental import pallas as pl
from jax.experimental.pallas import tpu as pltpu
from jax.sharding import PartitionSpec as P

epsilon = 1e-05
MESH = pl.DeviceIdType.MESH
F32 = jnp.float32
BF16 = jnp.bfloat16
LANES = 128


def dot(a, b):
    return jnp.dot(a, b, preferred_element_type=F32)


def layer_norm(values, gain, offset):
    centre = values - jnp.mean(values, axis=-1, keepdims=True)
    spread = jnp.mean(centre * centre, axis=-1, keepdims=True)
    return centre * lax.rsqrt(spread + epsilon) * gain + offset


def swish(v):
    h = 0.5 * v
    return (h * jnp.tanh(h) + h).astype(BF16)


def lanes_hot(column_sets):
    pieces = []
    lane = lax.broadcasted_iota(jnp.int32, (LANES, LANES), 1)
    for group, columns in enumerate(column_sets):
        places = lane + group * LANES
        hit = places == columns[0]
        for other in columns[1:]:
            hit = hit | (places == other)
        pieces.append(jnp.where(hit, 1.0, 0.0).astype(BF16))
    return jnp.concatenate(pieces, axis=1)


def rows_hot(row, height):
    places = lax.broadcasted_iota(jnp.int32, (height, row.shape[1]), 0)
    return jnp.where(places == row, 1.0, 0.0).astype(BF16)


def lists_hot(lists, nodes):
    slots, shards = lists.shape
    rows = shards * slots
    row_place = lax.broadcasted_iota(jnp.int32, (rows, shards), 0)
    shard_place = lax.broadcasted_iota(jnp.int32, (rows, shards), 1)
    spread = jnp.where(lax.div(row_place, slots) == shard_place, 1.0, 0.0).astype(BF16)
    contract = (((1,), (1,)), ((), ()))

    def over(part):
        return lax.dot_general(spread, part.astype(F32).astype(BF16), contract, preferred_element_type=F32)

    picked = over(jnp.right_shift(lists, 4)) * 16.0 + over(jnp.bitwise_and(lists, 15))
    place = lax.rem(lax.broadcasted_iota(jnp.int32, picked.shape, 0), slots)
    slot_place = lax.broadcasted_iota(jnp.int32, picked.shape, 1)
    wanted = jnp.sum(jnp.where(place == slot_place, picked, 0.0), axis=1, keepdims=True)
    node_place = lax.broadcasted_iota(jnp.int32, (rows, nodes), 1).astype(F32)
    return jnp.where(node_place == wanted, 1.0, 0.0).astype(BF16)


def finish(
    chunks, chunk, counts_ref, pre, halo_hot, halo_table, second, gain, offset,
    state, low, low_row, scatter_hot, hidden, summed, emit,
):
    blocks = chunk // LANES
    places = lax.broadcasted_iota(jnp.int32, (LANES, state.shape[1]), 0)

    def part(c):
        return pl.ds(c * chunk, chunk)

    def gather(c):
        hidden[c % 2] = swish(dot(halo_hot[part(c), :], halo_table) + pre[part(c), :])

    def renew(c):
        update = layer_norm(dot(hidden[c % 2], second), gain, offset)
        for i in range(blocks):
            here = pl.ds(c * chunk + i * LANES, LANES)
            kept = jnp.where(places < counts_ref[c * blocks + i], update[i * LANES : (i + 1) * LANES], 0.0)
            fresh = state[here, :] + kept
            low[pl.ds(low_row(c) + i * LANES, LANES), :] = fresh.astype(BF16)
            emit(here, fresh)

    def scatter(c):
        added = dot(scatter_hot[:, part(c)], low[pl.ds(low_row(c), chunk), :])
        summed[...] = added if c == 0 else summed[...] + added

    for step in range(chunks + 2):
        if 1 <= step <= chunks:
            renew(step - 1)
        if step < chunks:
            gather(step)
        if step >= 2:
            scatter(step - 2)


def node_step(node_pre, summed, first, second, gain, offset):
    v = node_pre + dot(summed.astype(BF16), first)
    return layer_norm(dot(swish(v), second), gain, offset)


def first_kernel(
    patches, bands, chunk,
    counts_hbm, lat_hbm, senders_hbm, receivers_hbm, lists_hbm, eb_hbm, eg_hbm, eo_hbm, nb_hbm, ng_hbm, no_hbm,
    edge_hbm, ew1_hbm, ew2_hbm, nw1_hbm, nw2_hbm,
    state, pre, halo_hot, scatter_hot, table_out, node_out, node_pre, w2_out, v1_out, v2_out,
    counts_ref, lat_ref, senders_ref, receivers_ref, lists_in, eb_ref, eg_ref, eo_ref, nb_ref, ng_ref, no_ref,
    w1, w2, v1, v2, x1, own_lists, node_hot, table, low, hidden, low_out, rest_out, low_in, rest_in,
    out_a, in_a, out_b, in_b, summed,
    load_sem, list_send, list_recv, low_send, low_recv, rest_send, rest_recv, send_a, recv_a, send_b, recv_b,
):
    shards = patches * bands
    patch, band = lax.axis_index("patch"), lax.axis_index("band")
    me = patch * bands + band
    nodes = node_out.shape[0]
    edges, width = state.shape
    half = lat_ref.shape[1]
    chunks = edges // chunk
    blocks = edges // LANES
    slot = out_b.shape[1]

    loads = [
        pltpu.make_async_copy(src, dst, load_sem.at[i])
        for i, (src, dst) in enumerate((
            (lists_hbm.at[0], lists_in.at[band]), (lat_hbm, lat_ref), (counts_hbm, counts_ref),
            (senders_hbm, senders_ref), (receivers_hbm, receivers_ref),
            (edge_hbm, state), (ew1_hbm.at[0], w1), (eb_hbm, eb_ref),
            (ew2_hbm.at[0], w2), (nw1_hbm.at[0], v1), (nw2_hbm.at[0], v2),
            (eg_hbm, eg_ref), (eo_hbm, eo_ref), (nb_hbm, nb_ref), (ng_hbm, ng_ref), (no_hbm, no_ref),
            (ew1_hbm.at[1], x1), (ew2_hbm.at[1], w2_out),
            (nw1_hbm.at[1], v1_out), (nw2_hbm.at[1], v2_out),
        ))
    ]
    for load in loads:
        load.start()

    def place(q):
        return (lax.div(q, bands), lax.rem(q, bands))

    barrier = pltpu.get_barrier_semaphore()
    for i in range(1, bands):
        pl.semaphore_signal(barrier, inc=1, device_id=(patch, lax.rem(band + i, bands)), device_id_type=MESH)

    def greet(i, c):
        other = lax.rem(patch + i, patches)
        for j in range(bands):
            pl.semaphore_signal(barrier, inc=1, device_id=(other, j), device_id_type=MESH)
        return c

    lax.fori_loop(1, patches, greet, 0)
    loads[0].wait()
    loads[1].wait()
    for c in range(bands):
        rows = lat_ref[c * nodes : (c + 1) * nodes, :]
        low_out[c] = rows.astype(BF16)
        rest_out[c] = (rows - low_out[c].astype(F32)).astype(BF16)
    low_in[band] = low_out[band]
    rest_in[band] = rest_out[band]
    pl.semaphore_wait(barrier, shards - 1)

    def exchange(source, target, ss, rs):
        return [
            pltpu.make_async_remote_copy(
                src_ref=source(lax.rem(band + i, bands)), dst_ref=target, send_sem=ss.at[i], recv_sem=rs.at[i],
                device_id=(patch, lax.rem(band + i, bands)), device_id_type=MESH,
            )
            for i in range(1, bands)
        ]

    list_copies = exchange(lambda other: lists_in.at[band], lists_in.at[band], list_send, list_recv)
    low_copies = exchange(lambda other: low_out.at[other], low_in.at[band], low_send, low_recv)
    rest_copies = exchange(lambda other: rest_out.at[other], rest_in.at[band], rest_send, rest_recv)
    for copy in list_copies:
        copy.start()

    def to_all(source, target, ss, rs):
        def go(k, c):
            q = lax.rem(me + k, shards)
            pltpu.make_async_remote_copy(
                src_ref=source.at[q], dst_ref=target, send_sem=ss, recv_sem=rs,
                device_id=place(q), device_id_type=MESH,
            ).start()
            return c

        lax.fori_loop(1, shards, go, 0)

    def from_all(source, target, ss, rs):
        others = pl.ds(0, shards - 1)
        pltpu.make_async_remote_copy(
            src_ref=source.at[others], dst_ref=target.at[others], send_sem=ss, recv_sem=rs,
            device_id=(patch, lax.rem(band + 1, bands)), device_id_type=MESH,
        ).wait()

    def send_band(i):
        owner = lax.rem(band + i, bands)
        hot = lists_hot(lists_in[owner], nodes)
        if i == 0:
            own_lists[...] = hot
        sender = patch * bands + owner
        out_a[i] = dot(hot, low_out[owner]).reshape(shards, slot, half).astype(BF16)
        in_a[band, sender] = out_a[i, me]
        to_all(out_a.at[i], in_a.at[band, sender], send_a.at[i], recv_a.at[i])

    send_band(0)
    for copy in low_copies:
        copy.start()
    for i in range(1, bands):
        list_copies[i - 1].wait()
        send_band(i)
    for copy in rest_copies:
        copy.start()

    def part(c):
        return pl.ds(pl.multiple_of(c * chunk, chunk), chunk)

    for load in loads[2:8]:
        load.wait()

    def own_edges(c, carry):
        pre[part(c), :] = dot(state[part(c), :].astype(BF16), w1[0:width, :]) + eb_ref[0:1, :]
        return carry

    lax.fori_loop(0, chunks, own_edges, 0)

    def columns_of(ref):
        rows = [ref[pl.ds(j * LANES, LANES)].reshape(1, LANES) for j in range(blocks)]
        return jnp.concatenate(rows + [jnp.zeros((LANES - blocks, LANES), jnp.int32)], axis=0).T

    sender_columns, receiver_columns = columns_of(senders_ref), columns_of(receivers_ref)
    edge_place = lax.broadcasted_iota(jnp.int32, (1, LANES), 1)
    for j in range(blocks):
        here = slice(j * LANES, (j + 1) * LANES)
        sender = jnp.broadcast_to(sender_columns[:, j : j + 1], (LANES, LANES))
        receiver = jnp.broadcast_to(receiver_columns[:, j : j + 1], (LANES, LANES)) + nodes
        local, beyond = jnp.where(sender < nodes, sender, -1), sender - nodes
        sets = []
        for first in range(0, 2 * nodes, LANES):
            sets.append([local] * (first < nodes) + [receiver] * (first + LANES > nodes))
        node_hot[here, :] = lanes_hot(sets)
        halo_hot[here, :] = lanes_hot([[beyond]] * (halo_hot.shape[1] // LANES))
        row = receivers_ref[pl.ds(j * LANES, LANES)].reshape(1, LANES)
        scatter_hot[:, here] = rows_hot(jnp.where(edge_place < counts_ref[j], row, -1), nodes)

    for copy in low_copies:
        copy.wait()
    node_low = jnp.concatenate([low_in[i] for i in range(bands)], axis=1)
    table[0:nodes, :] = dot(node_low, w1[width : 2 * width, :]).astype(BF16)
    table[nodes:, :] = dot(node_low, w1[2 * width :, :]).astype(BF16)

    def own_nodes(c, carry):
        pre[part(c), :] += dot(node_hot[part(c), :], table[...])
        return carry

    lax.fori_loop(0, chunks, own_nodes, 0)
    for load in loads[8:]:
        load.wait()
    node_pre[...] = dot(node_low, v1[0:width, :]) + nb_ref[0:1, :]
    for i in range(bands):
        from_all(out_a.at[i], in_a.at[0], send_a.at[i], recv_a.at[i])

    def flat(values):
        return values.astype(F32).reshape(shards * slot, values.shape[2]).astype(BF16)

    halo = jnp.concatenate([flat(in_a[i]) for i in range(bands)], axis=1)
    table_out[...] = dot(halo, w1[width : 2 * width, :]).astype(BF16)

    def keep(here, fresh):
        state[here, :] = fresh

    finish(
        chunks, chunk, counts_ref, pre, halo_hot, table_out[...], w2[...], eg_ref[0:1, :], eo_ref[0:1, :],
        state, low, lambda c: c * chunk, scatter_hot, hidden, summed, keep,
    )
    for copy in rest_copies:
        copy.wait()
    wide = [low_in[i].astype(F32) + rest_in[i].astype(F32) for i in range(bands)]
    node_state = jnp.concatenate(wide, axis=1) + node_step(
        node_pre[...], summed[...], v1[width:, :], v2[...], ng_ref[0:1, :], no_ref[0:1, :]
    )
    node_out[...] = node_state
    node_low = node_state.astype(BF16)
    out_b[...] = dot(own_lists[...], node_low).reshape(shards, slot, width).astype(BF16)
    in_b[me] = out_b[me]
    to_all(out_b, in_b.at[me], send_b, recv_b)
    table[0:nodes, :] = dot(node_low, x1[width : 2 * width, :]).astype(BF16)
    table[nodes:, :] = dot(node_low, x1[2 * width :, :]).astype(BF16)
    node_pre[...] = dot(node_low, v1_out[0:width, :]) + nb_ref[1:2, :]

    def begin(c, carry):
        known = jnp.concatenate([low[part(c), :], node_hot[part(c), :]], axis=1)
        pre[part(c), :] = dot(known, jnp.concatenate([x1[0:width, :], table[...]], axis=0)) + eb_ref[1:2, :]
        return carry

    lax.fori_loop(0, chunks, begin, 0)
    from_all(out_b, in_b, send_b, recv_b)
    table_out[...] = dot(flat(in_b[...]), x1[width : 2 * width, :]).astype(BF16)


def second_kernel(
    chunk,
    counts_ref, state, pre, halo_hot, scatter_hot, table_ref, node_ref, node_pre, w2, v1, v2,
    eg_ref, eo_ref, ng_ref, no_ref,
    nodes_hbm, edges_hbm,
    nodes_out, edges_out, low, hidden, summed, store_sem,
):
    edges, width = state.shape
    chunks = edges // chunk
    blocks = edges // LANES
    stores = []

    def keep(here, fresh):
        edges_out[here, :] = fresh
        store = pltpu.make_async_copy(
            edges_out.at[here], edges_hbm.at[here], store_sem.at[len(stores)]
        )
        store.start()
        stores.append(store)

    finish(
        chunks, chunk, counts_ref, pre, halo_hot, table_ref[...], w2[...], eg_ref[1:2, :], eo_ref[1:2, :],
        state, low, lambda c: c % 2 * chunk, scatter_hot, hidden, summed, keep,
    )
    nodes_out[...] = node_ref[...] + node_step(
        node_pre[...], summed[...], v1[width:, :], v2[...], ng_ref[1:2, :], no_ref[1:2, :]
    )
    last = pltpu.make_async_copy(nodes_out, nodes_hbm, store_sem.at[blocks])
    last.start()
    for store in stores + [last]:
        store.wait()


def shards_body(
    patches, bands,
    latents, edge_latents, edge_sender, edge_receiver, block_counts, send_rows,
    edge_first_weight, edge_first_bias, edge_second_weight, edge_gain, edge_offset,
    node_first_weight, node_first_bias, node_second_weight, node_gain, node_offset,
):
    shards = patches * bands
    edges, width = edge_latents.shape
    nodes = latents.shape[0] // bands
    slot = send_rows.shape[2]
    half = latents.shape[1]
    chunk = next(c for c in (512, 256, 128) if edges % c == 0)
    scalars, far = pl.BlockSpec(memory_space=pltpu.SMEM), pl.BlockSpec(memory_space=pltpu.HBM)
    near = pl.BlockSpec(memory_space=pltpu.VMEM)
    dma = pltpu.SemaphoreType.DMA

    def shaped(*shape, kind=BF16):
        return jax.ShapeDtypeStruct(shape, kind)

    def held(*shape, kind=BF16):
        return pltpu.VMEM(shape, kind)

    def afar(array):
        return pltpu.with_memory_space_constraint(array, pltpu.HBM)

    handed = pl.pallas_call(
        functools.partial(first_kernel, patches, bands, chunk),
        out_shape=(
            held(edges, width, kind=F32),
            held(edges, width, kind=F32),
            held(edges, shards * slot),
            held(nodes, edges),
            held(shards * slot, width),
            held(nodes, width, kind=F32),
            held(nodes, width, kind=F32),
            held(*edge_second_weight.shape[1:]),
            held(*node_first_weight.shape[1:]),
            held(*node_second_weight.shape[1:]),
        ),
        in_specs=[far] * 16,
        out_specs=(near,) * 10,
        scratch_shapes=[
            pltpu.SMEM(block_counts.shape, jnp.int32),
            pltpu.VMEM(latents.shape, F32),
            pltpu.VMEM((edges,), jnp.int32),
            pltpu.VMEM((edges,), jnp.int32),
            pltpu.VMEM((bands, slot, shards), jnp.int32),
        ] + [pltpu.VMEM(edge_gain.shape, F32)] * 6 + [
            pltpu.VMEM(edge_first_weight.shape[1:], BF16),
            pltpu.VMEM(edge_second_weight.shape[1:], BF16),
            pltpu.VMEM(node_first_weight.shape[1:], BF16),
            pltpu.VMEM(node_second_weight.shape[1:], BF16),
            pltpu.VMEM(edge_first_weight.shape[1:], BF16),
            pltpu.VMEM((shards * slot, nodes), BF16),
            pltpu.VMEM((edges, 2 * nodes), BF16),
            pltpu.VMEM((2 * nodes, width), BF16),
            pltpu.VMEM((edges, width), BF16),
            pltpu.VMEM((2, chunk, width), BF16),
        ] + [pltpu.VMEM((bands, nodes, half), BF16)] * 4 + [
            pltpu.VMEM((bands, shards, slot, half), BF16),
            pltpu.VMEM((bands, shards, slot, half), BF16),
            pltpu.VMEM((shards, slot, width), BF16),
            pltpu.VMEM((shards, slot, width), BF16),
            pltpu.VMEM((nodes, width), F32),
            dma((20,)),
            dma((bands,)), dma((bands,)), dma((bands,)), dma((bands,)), dma((bands,)), dma((bands,)),
            dma((bands,)), dma((bands,)), dma, dma,
        ],
        compiler_params=pltpu.CompilerParams(
            collective_id=0, has_side_effects=True, vmem_limit_bytes=36 * 2**20
        ),
        name="layer_one",
    )(
        *map(afar, (
            block_counts, latents, edge_sender, edge_receiver, send_rows.transpose(0, 2, 1),
            edge_first_bias, edge_gain, edge_offset, node_first_bias, node_gain, node_offset,
            edge_latents, edge_first_weight, edge_second_weight, node_first_weight, node_second_weight,
        )),
    )
    return pl.pallas_call(
        functools.partial(second_kernel, chunk),
        out_shape=(shaped(nodes, width, kind=F32), shaped(edges, width, kind=F32)),
        in_specs=[scalars] + [near] * 14,
        out_specs=(far, far),
        scratch_shapes=[
            pltpu.VMEM((nodes, width), F32),
            pltpu.VMEM((edges, width), F32),
            pltpu.VMEM((2 * chunk, width), BF16),
            pltpu.VMEM((2, chunk, width), BF16),
            pltpu.VMEM((nodes, width), F32),
            dma((edges // LANES + 1,)),
        ],
        compiler_params=pltpu.CompilerParams(vmem_limit_bytes=24 * 2**20),
        name="layer_two",
    )(block_counts, *handed, edge_gain, edge_offset, node_gain, node_offset)


def solution(mesh):
    owned = P(("patch", "band"))
    return jax.shard_map(
        functools.partial(shards_body, mesh.shape["patch"], mesh.shape["band"]),
        mesh=mesh,
        in_specs=(P("patch", "band"), owned, owned, owned, owned, owned) + (P(),) * 10,
        out_specs=(owned, owned),
        check_vma=False,
    )
```

```python
import functools

import jax
import jax.numpy as jnp
from jax import lax
from jax.experimental import pallas as pl
from jax.experimental.pallas import tpu as pltpu
from jax.sharding import PartitionSpec as P

epsilon = 1e-05
MESH = pl.DeviceIdType.MESH
F32 = jnp.float32
BF16 = jnp.bfloat16
LANES = 128


def dot(a, b):
    return jnp.dot(a, b, preferred_element_type=F32)


def layer_norm(values, gain, offset):
    centre = values - jnp.mean(values, axis=-1, keepdims=True)
    spread = jnp.mean(centre * centre, axis=-1, keepdims=True)
    return centre * lax.rsqrt(spread + epsilon) * gain + offset


def swish(h):
    return (h * jnp.tanh(h) + h).astype(BF16)


def pair_of(index):
    low, high = jnp.bitwise_and(index, LANES - 1), jnp.right_shift(index, 7)
    return low.astype(F32).astype(BF16), high.astype(F32).astype(BF16)


def spread(pair, column):
    return [jnp.broadcast_to(part[:, column : column + 1], (LANES, LANES)) for part in pair]


def groups_hot(low, high, places, groups):
    one, none = jnp.ones(places.shape, BF16), jnp.zeros(places.shape, BF16)
    base = jnp.where(low == places, one, none)
    return [jnp.where(high == jnp.full(places.shape, g, BF16), base, none) for g in groups]


def lists_hot(lists, nodes):
    slots, shards = lists.shape
    place = lax.broadcasted_iota(jnp.int32, (slots, nodes), 1)
    rows = [
        jnp.where(place == jnp.broadcast_to(lists[:, q : q + 1], (slots, nodes)), 1.0, 0.0) for q in range(shards)
    ]
    return jnp.concatenate(rows, axis=0).astype(BF16)


def finish(
    chunks, chunk, counts_ref, pre, halo_hot, halo_table, second, gain,
    base, low, low_row, scatter_hot, hidden, summed, emit,
):
    blocks = chunk // LANES
    places = lax.broadcasted_iota(jnp.int32, (LANES, 1), 0)

    def part(c):
        return pl.ds(c * chunk, chunk)

    def gather(c):
        hidden[c % 2] = swish(dot(halo_hot[part(c), :], halo_table) + pre[part(c), :])

    def renew(c):
        values = dot(hidden[c % 2], second)
        centre = values - jnp.mean(values, axis=-1, keepdims=True)
        scale = lax.rsqrt(jnp.mean(centre * centre, axis=-1, keepdims=True) + epsilon)
        for i in range(blocks):
            here, rows = pl.ds(c * chunk + i * LANES, LANES), slice(i * LANES, (i + 1) * LANES)
            kept = jnp.where(places < counts_ref[c * blocks + i], scale[rows], 0.0)
            fresh = base[here, :] + centre[rows] * kept * gain
            low[pl.ds(low_row(c) + i * LANES, LANES), :] = fresh.astype(BF16)
            emit(here, fresh)

    def scatter(c):
        added = dot(scatter_hot[:, part(c)], low[pl.ds(low_row(c), chunk), :])
        summed[...] = added if c == 0 else summed[...] + added

    for step in range(chunks + 2):
        if 1 <= step <= chunks:
            renew(step - 1)
        if step < chunks:
            gather(step)
        if step >= 2:
            scatter(step - 2)


def node_step(node_pre, summed, first, second, gain, offset):
    h = node_pre + 0.5 * dot(summed.astype(BF16), first)
    return layer_norm(dot(swish(h), second), gain, offset)


def with_offset(state, counts_ref, first, offset):
    places = lax.broadcasted_iota(jnp.int32, (LANES, 1), 0)
    pieces = []
    for i in range(state.shape[0] // LANES):
        usable = places < counts_ref[first + i]
        pieces.append(state[i * LANES : (i + 1) * LANES] + jnp.where(usable, offset, 0.0))
    return jnp.concatenate(pieces, axis=0)


def first_kernel(
    patches, bands, chunk,
    counts_hbm, lat_hbm, senders_hbm, receivers_hbm, lists_hbm, eb_hbm, eg_hbm, eo_hbm, nb_hbm, ng_hbm, no_hbm,
    edge_hbm, ew1_hbm, ew2_hbm, nw1_hbm, nw2_hbm,
    state, pre, halo_hot, scatter_hot, table_out, node_out, node_pre, w2_out, v1_out, v2_out,
    counts_ref, lat_ref, senders_ref, receivers_ref, lists_in, eb_ref, eg_ref, eo_ref, nb_ref, ng_ref, no_ref,
    w1, w2, v1, v2, x1, own_lists, node_hot, table, low, hidden, low_out, rest_out, low_in, rest_in,
    out_a, in_a, out_b, in_b, summed,
    load_sem, list_send, list_recv, low_send, low_recv, rest_send, rest_recv, send_a, recv_a, send_b, recv_b,
):
    shards = patches * bands
    patch, band = lax.axis_index("patch"), lax.axis_index("band")
    me = patch * bands + band
    nodes = node_out.shape[0]
    edges, width = state.shape
    half = lat_ref.shape[1]
    chunks = edges // chunk
    blocks = edges // LANES
    slot = out_b.shape[1]

    loads = [
        pltpu.make_async_copy(src, dst, load_sem.at[i])
        for i, (src, dst) in enumerate((
            (lists_hbm.at[0], lists_in.at[band]), (lat_hbm, lat_ref), (counts_hbm, counts_ref),
            (senders_hbm, senders_ref), (receivers_hbm, receivers_ref),
            (edge_hbm, state), (ew1_hbm.at[0], w1), (eb_hbm, eb_ref),
            (ew2_hbm.at[0], w2), (nw1_hbm.at[0], v1), (nw2_hbm.at[0], v2),
            (eg_hbm, eg_ref), (eo_hbm, eo_ref), (nb_hbm, nb_ref), (ng_hbm, ng_ref), (no_hbm, no_ref),
            (ew1_hbm.at[1], x1), (ew2_hbm.at[1], w2_out),
            (nw1_hbm.at[1], v1_out), (nw2_hbm.at[1], v2_out),
        ))
    ]
    for load in loads:
        load.start()

    def place(q):
        return (lax.div(q, bands), lax.rem(q, bands))

    barrier = pltpu.get_barrier_semaphore()
    for i in range(1, bands):
        pl.semaphore_signal(barrier, inc=1, device_id=(patch, lax.rem(band + i, bands)), device_id_type=MESH)

    def greet(i, c):
        other = lax.rem(patch + i, patches)
        for j in range(bands):
            pl.semaphore_signal(barrier, inc=1, device_id=(other, j), device_id_type=MESH)
        return c

    lax.fori_loop(1, patches, greet, 0)
    loads[0].wait()
    loads[1].wait()
    for c in range(bands):
        rows = lat_ref[c * nodes : (c + 1) * nodes, :]
        low_out[c] = rows.astype(BF16)
        rest_out[c] = (rows - low_out[c].astype(F32)).astype(BF16)
    low_in[band] = low_out[band]
    rest_in[band] = rest_out[band]

    def pick_band(i):
        owner = lax.rem(band + i, bands)
        hot = lists_hot(lists_in[owner], nodes)
        if i == 0:
            own_lists[...] = hot
        out_a[i] = dot(hot, low_out[owner]).reshape(shards, slot, half).astype(BF16)
        in_a[band, patch * bands + owner] = out_a[i, me]

    pick_band(0)
    pl.semaphore_wait(barrier, shards - 1)

    def exchange(source, target, ss, rs):
        return [
            pltpu.make_async_remote_copy(
                src_ref=source(lax.rem(band + i, bands)), dst_ref=target, send_sem=ss.at[i], recv_sem=rs.at[i],
                device_id=(patch, lax.rem(band + i, bands)), device_id_type=MESH,
            )
            for i in range(1, bands)
        ]

    list_copies = exchange(lambda other: lists_in.at[band], lists_in.at[band], list_send, list_recv)
    low_copies = exchange(lambda other: low_out.at[other], low_in.at[band], low_send, low_recv)
    rest_copies = exchange(lambda other: rest_out.at[other], rest_in.at[band], rest_send, rest_recv)
    for copy in list_copies:
        copy.start()

    def to_all(source, target, ss, rs):
        def go(k, c):
            q = lax.rem(me + k, shards)
            pltpu.make_async_remote_copy(
                src_ref=source.at[q], dst_ref=target, send_sem=ss, recv_sem=rs,
                device_id=place(q), device_id_type=MESH,
            ).start()
            return c

        lax.fori_loop(1, shards, go, 0)

    def from_all(source, target, ss, rs):
        others = pl.ds(0, shards - 1)
        pltpu.make_async_remote_copy(
            src_ref=source.at[others], dst_ref=target.at[others], send_sem=ss, recv_sem=rs,
            device_id=(patch, lax.rem(band + 1, bands)), device_id_type=MESH,
        ).wait()

    def send_band(i):
        sender = patch * bands + lax.rem(band + i, bands)
        to_all(out_a.at[i], in_a.at[band, sender], send_a.at[i], recv_a.at[i])

    for copy in low_copies:
        copy.start()
    send_band(0)

    def part(c):
        return slice(c * chunk, (c + 1) * chunk)

    for load in loads[2:8]:
        load.wait()

    def matrix_of(ref):
        rows = [ref[pl.ds(j * LANES, LANES)].reshape(1, LANES) for j in range(blocks)]
        return jnp.concatenate(rows + [jnp.zeros((LANES - blocks, LANES), jnp.int32)], axis=0)

    senders, receivers = matrix_of(senders_ref).T, matrix_of(receivers_ref).T
    local_pair = pair_of(jnp.where(senders < nodes, senders, -1))
    halo_pair = pair_of(senders - nodes)
    receiver_pair = pair_of(receivers + nodes)
    lane = lax.broadcasted_iota(jnp.int32, (LANES, LANES), 1).astype(F32).astype(BF16)
    row_place = lax.broadcasted_iota(jnp.int32, (LANES, LANES), 0).astype(F32).astype(BF16)
    edge_place = lax.broadcasted_iota(jnp.int32, (1, LANES), 1)
    first_receiver, node_groups = nodes // LANES, 2 * nodes // LANES
    last_local = (nodes - 1) // LANES

    def build_hot(j):
        here = slice(j * LANES, (j + 1) * LANES)
        local = groups_hot(*spread(local_pair, j), lane, range(last_local + 1))
        entering = groups_hot(*spread(receiver_pair, j), lane, range(first_receiver, node_groups))
        for g in range(node_groups):
            shown = [x for x in (
                local[g] if g <= last_local else None, entering[g - first_receiver] if g >= first_receiver else None
            ) if x is not None]
            node_hot[here, g * LANES : (g + 1) * LANES] = sum(shown[1:], shown[0])
        beyond = groups_hot(*spread(halo_pair, j), lane, range(halo_hot.shape[1] // LANES))
        halo_hot[here, :] = jnp.concatenate(beyond, axis=1)
        row = jnp.where(edge_place < counts_ref[j], receivers_ref[pl.ds(j * LANES, LANES)].reshape(1, LANES), -1)
        low_row, high_row = [jnp.broadcast_to(x, (LANES, LANES)) for x in pair_of(row)]
        for g, hot in enumerate(groups_hot(low_row, high_row, row_place, range(last_local + 1))):
            rows = min(LANES, nodes - g * LANES)
            scatter_hot[g * LANES : g * LANES + rows, here] = hot[0:rows]

    for c in range(chunks):
        pre[part(c), :] = dot(state[part(c), :].astype(BF16), w1[0:width, :]) + eb_ref[0:1, :]
        for j in range(c * chunk // LANES, (c + 1) * chunk // LANES):
            build_hot(j)

    for i in range(1, bands):
        list_copies[i - 1].wait()
        pick_band(i)
        send_band(i)
    for copy in low_copies:
        copy.wait()
    for copy in rest_copies:
        copy.start()
    node_low = jnp.concatenate([low_in[i] for i in range(bands)], axis=1)
    table[0:nodes, :] = dot(node_low, w1[width : 2 * width, :]).astype(BF16)
    table[nodes:, :] = dot(node_low, w1[2 * width :, :]).astype(BF16)

    for load in loads[8:]:
        load.wait()
    for c in range(chunks):
        pre[part(c), :] = 0.5 * (pre[part(c), :] + dot(node_hot[part(c), :], table[...]))
        state[part(c), :] = with_offset(state[part(c), :], counts_ref, c * chunk // LANES, eo_ref[0:1, :])
    node_pre[...] = 0.5 * (dot(node_low, v1[0:width, :]) + nb_ref[0:1, :])
    for i in range(bands):
        from_all(out_a.at[i], in_a.at[0], send_a.at[i], recv_a.at[i])

    def flat(values):
        return values.astype(F32).reshape(shards * slot, values.shape[2]).astype(BF16)

    halo = jnp.concatenate([flat(in_a[i]) for i in range(bands)], axis=1)
    table_out[...] = (0.5 * dot(halo, w1[width : 2 * width, :])).astype(BF16)

    def keep(here, fresh):
        state[here, :] = fresh

    finish(
        chunks, chunk, counts_ref, pre, halo_hot, table_out[...], w2[...], eg_ref[0:1, :],
        state, low, lambda c: c * chunk, scatter_hot, hidden, summed, keep,
    )
    for copy in rest_copies:
        copy.wait()
    wide = [low_in[i].astype(F32) + rest_in[i].astype(F32) for i in range(bands)]
    node_state = jnp.concatenate(wide, axis=1) + node_step(
        node_pre[...], summed[...], v1[width:, :], v2[...], ng_ref[0:1, :], no_ref[0:1, :]
    )
    node_out[...] = node_state
    node_low = node_state.astype(BF16)
    out_b[...] = dot(own_lists[...], node_low).reshape(shards, slot, width).astype(BF16)
    in_b[me] = out_b[me]
    to_all(out_b, in_b.at[me], send_b, recv_b)
    table[0:nodes, :] = dot(node_low, x1[width : 2 * width, :]).astype(BF16)
    table[nodes:, :] = dot(node_low, x1[2 * width :, :]).astype(BF16)
    node_pre[...] = 0.5 * (dot(node_low, v1_out[0:width, :]) + nb_ref[1:2, :])
    known_weight = jnp.concatenate([x1[0:width, :], table[...]], axis=0)
    for c in range(chunks):
        known = jnp.concatenate([low[part(c), :], node_hot[part(c), :]], axis=1)
        pre[part(c), :] = 0.5 * (dot(known, known_weight) + eb_ref[1:2, :])
        state[part(c), :] = with_offset(state[part(c), :], counts_ref, c * chunk // LANES, eo_ref[1:2, :])
    from_all(out_b, in_b, send_b, recv_b)
    table_out[...] = (0.5 * dot(flat(in_b[...]), x1[width : 2 * width, :])).astype(BF16)


def second_kernel(
    chunk,
    counts_ref, state, pre, halo_hot, scatter_hot, table_ref, node_ref, node_pre, w2, v1, v2,
    eg_ref, ng_ref, no_ref,
    nodes_hbm, edges_hbm,
    nodes_out, edges_out, low, hidden, summed, store_sem,
):
    edges, width = state.shape
    chunks = edges // chunk
    blocks = edges // LANES
    stores = []

    def keep(here, fresh):
        edges_out[here, :] = fresh
        store = pltpu.make_async_copy(
            edges_out.at[here], edges_hbm.at[here], store_sem.at[len(stores)]
        )
        store.start()
        stores.append(store)

    finish(
        chunks, chunk, counts_ref, pre, halo_hot, table_ref[...], w2[...], eg_ref[1:2, :],
        state, low, lambda c: c % 2 * chunk, scatter_hot, hidden, summed, keep,
    )
    nodes_out[...] = node_ref[...] + node_step(
        node_pre[...], summed[...], v1[width:, :], v2[...], ng_ref[1:2, :], no_ref[1:2, :]
    )
    last = pltpu.make_async_copy(nodes_out, nodes_hbm, store_sem.at[blocks])
    last.start()
    for store in stores + [last]:
        store.wait()


def shards_body(
    patches, bands,
    latents, edge_latents, edge_sender, edge_receiver, block_counts, send_rows,
    edge_first_weight, edge_first_bias, edge_second_weight, edge_gain, edge_offset,
    node_first_weight, node_first_bias, node_second_weight, node_gain, node_offset,
):
    shards = patches * bands
    edges, width = edge_latents.shape
    nodes = latents.shape[0] // bands
    slot = send_rows.shape[2]
    half = latents.shape[1]
    chunk = next(c for c in (512, 256, 128) if edges % c == 0)
    scalars, far = pl.BlockSpec(memory_space=pltpu.SMEM), pl.BlockSpec(memory_space=pltpu.HBM)
    near = pl.BlockSpec(memory_space=pltpu.VMEM)
    dma = pltpu.SemaphoreType.DMA

    def shaped(*shape, kind=BF16):
        return jax.ShapeDtypeStruct(shape, kind)

    def held(*shape, kind=BF16):
        return pltpu.VMEM(shape, kind)

    def afar(array):
        return pltpu.with_memory_space_constraint(array, pltpu.HBM)

    handed = pl.pallas_call(
        functools.partial(first_kernel, patches, bands, chunk),
        out_shape=(
            held(edges, width, kind=F32),
            held(edges, width, kind=F32),
            held(edges, shards * slot),
            held(nodes, edges),
            held(shards * slot, width),
            held(nodes, width, kind=F32),
            held(nodes, width, kind=F32),
            held(*edge_second_weight.shape[1:]),
            held(*node_first_weight.shape[1:]),
            held(*node_second_weight.shape[1:]),
        ),
        in_specs=[far] * 16,
        out_specs=(near,) * 10,
        scratch_shapes=[
            pltpu.SMEM(block_counts.shape, jnp.int32),
            pltpu.VMEM(latents.shape, F32),
            pltpu.VMEM((edges,), jnp.int32),
            pltpu.VMEM((edges,), jnp.int32),
            pltpu.VMEM((bands, slot, shards), jnp.int32),
        ] + [pltpu.VMEM(edge_gain.shape, F32)] * 6 + [
            pltpu.VMEM(edge_first_weight.shape[1:], BF16),
            pltpu.VMEM(edge_second_weight.shape[1:], BF16),
            pltpu.VMEM(node_first_weight.shape[1:], BF16),
            pltpu.VMEM(node_second_weight.shape[1:], BF16),
            pltpu.VMEM(edge_first_weight.shape[1:], BF16),
            pltpu.VMEM((shards * slot, nodes), BF16),
            pltpu.VMEM((edges, 2 * nodes), BF16),
            pltpu.VMEM((2 * nodes, width), BF16),
            pltpu.VMEM((edges, width), BF16),
            pltpu.VMEM((2, chunk, width), BF16),
        ] + [pltpu.VMEM((bands, nodes, half), BF16)] * 4 + [
            pltpu.VMEM((bands, shards, slot, half), BF16),
            pltpu.VMEM((bands, shards, slot, half), BF16),
            pltpu.VMEM((shards, slot, width), BF16),
            pltpu.VMEM((shards, slot, width), BF16),
            pltpu.VMEM((nodes, width), F32),
            dma((20,)),
            dma((bands,)), dma((bands,)), dma((bands,)), dma((bands,)), dma((bands,)), dma((bands,)),
            dma((bands,)), dma((bands,)), dma, dma,
        ],
        compiler_params=pltpu.CompilerParams(
            collective_id=0, has_side_effects=True, vmem_limit_bytes=36 * 2**20
        ),
        name="layer_one",
    )(
        *map(afar, (
            block_counts, latents, edge_sender, edge_receiver, send_rows.transpose(0, 2, 1),
            edge_first_bias, edge_gain, edge_offset, node_first_bias, node_gain, node_offset,
            edge_latents, edge_first_weight, edge_second_weight, node_first_weight, node_second_weight,
        )),
    )
    return pl.pallas_call(
        functools.partial(second_kernel, chunk),
        out_shape=(shaped(nodes, width, kind=F32), shaped(edges, width, kind=F32)),
        in_specs=[scalars] + [near] * 13,
        out_specs=(far, far),
        scratch_shapes=[
            pltpu.VMEM((nodes, width), F32),
            pltpu.VMEM((edges, width), F32),
            pltpu.VMEM((2 * chunk, width), BF16),
            pltpu.VMEM((2, chunk, width), BF16),
            pltpu.VMEM((nodes, width), F32),
            dma((edges // LANES + 1,)),
        ],
        compiler_params=pltpu.CompilerParams(vmem_limit_bytes=24 * 2**20),
        name="layer_two",
    )(block_counts, *handed, edge_gain, node_gain, node_offset)


def solution(mesh):
    owned = P(("patch", "band"))
    return jax.shard_map(
        functools.partial(shards_body, mesh.shape["patch"], mesh.shape["band"]),
        mesh=mesh,
        in_specs=(P("patch", "band"), owned, owned, owned, owned, owned) + (P(),) * 10,
        out_specs=(owned, owned),
        check_vma=False,
    )
```

```python
import functools

import jax
import jax.numpy as jnp
from jax import lax
from jax.experimental import pallas as pl
from jax.experimental.pallas import tpu as pltpu
from jax.sharding import PartitionSpec as P

epsilon = 1e-05
MESH = pl.DeviceIdType.MESH
F32 = jnp.float32
BF16 = jnp.bfloat16
LANES = 128


def dot(a, b):
    return jnp.dot(a, b, preferred_element_type=F32)


def centred(values):
    return values - jnp.mean(values, axis=-1, keepdims=True)


def inverse_spread(centre):
    return lax.rsqrt(jnp.mean(centre * centre, axis=-1, keepdims=True) + epsilon)


def swish(h):
    return (h * jnp.tanh(h) + h).astype(BF16)


def pair_of(index):
    low, high = jnp.bitwise_and(index, LANES - 1), jnp.right_shift(index, 7)
    return low.astype(F32).astype(BF16), high.astype(F32).astype(BF16)


def spread(pair, column):
    return [jnp.broadcast_to(part[:, column : column + 1], (LANES, LANES)) for part in pair]


def groups_hot(low, high, places, groups):
    one, none = jnp.ones(places.shape, BF16), jnp.zeros(places.shape, BF16)
    base = jnp.where(low == places, one, none)
    return [jnp.where(high == jnp.full(places.shape, g, BF16), base, none) for g in groups]


def lists_hot(lists, nodes):
    slots, shards = lists.shape
    place = lax.broadcasted_iota(jnp.int32, (slots, nodes), 1)
    rows = [
        jnp.where(place == jnp.broadcast_to(lists[:, q : q + 1], (slots, nodes)), 1.0, 0.0) for q in range(shards)
    ]
    return jnp.concatenate(rows, axis=0).astype(BF16)


def finish(
    chunks, chunk, usable, pre, halo_hot, halo_table, second, gain,
    base, low, low_row, scatter_hot, hidden, summed, emit,
):
    groups = base.shape[1] // LANES

    def part(c):
        return pl.ds(c * chunk, chunk)

    def gather(c):
        hidden[c % 2] = swish(dot(halo_hot[part(c), :], halo_table) + pre[part(c), :])

    def renew(c):
        centre = centred(dot(hidden[c % 2], second))
        kept = inverse_spread(centre) * usable[part(c), :]
        fresh = base[part(c), :] + centre * jnp.concatenate([kept] * groups, axis=1) * gain
        low[pl.ds(low_row(c), chunk), :] = fresh.astype(BF16)
        emit(part(c), fresh)

    def scatter(c):
        added = dot(scatter_hot[:, part(c)], low[pl.ds(low_row(c), chunk), :])
        summed[...] = added if c == 0 else summed[...] + added

    for step in range(chunks + 2):
        if 1 <= step <= chunks:
            renew(step - 1)
        if step < chunks:
            gather(step)
        if step >= 2:
            scatter(step - 2)


def node_step(node_pre, summed, first, second, gain, offset):
    h = node_pre + 0.5 * dot(summed.astype(BF16), first)
    centre = centred(dot(swish(h), second))
    return centre * inverse_spread(centre) * gain + offset


def with_offset(state, usable, offset):
    return state + jnp.concatenate([usable] * (state.shape[1] // LANES), axis=1) * offset


def first_kernel(
    patches, bands, chunk,
    counts_hbm, lat_hbm, senders_hbm, receivers_hbm, lists_hbm, eb_hbm, eg_hbm, eo_hbm, nb_hbm, ng_hbm, no_hbm,
    edge_hbm, ew1_hbm, ew2_hbm, nw1_hbm, nw2_hbm,
    state, pre, usable, halo_hot, scatter_hot, table_out, node_out, node_pre, w2_out, v1_out, v2_out,
    counts_ref, lat_ref, senders_ref, receivers_ref, lists_in, eb_ref, eg_ref, eo_ref, nb_ref, ng_ref, no_ref,
    w1, w2, v1, v2, x1, own_lists, node_hot, table, partial, low, hidden, low_out, rest_out, low_in, rest_in,
    out_a, in_a, out_b, in_b, summed,
    load_sem, list_send, list_recv, low_send, low_recv, rest_send, rest_recv, send_a, recv_a, send_b, recv_b,
):
    shards = patches * bands
    patch, band = lax.axis_index("patch"), lax.axis_index("band")
    me = patch * bands + band
    nodes = node_out.shape[0]
    edges, width = state.shape
    half = lat_ref.shape[1]
    chunks = edges // chunk
    blocks = edges // LANES
    slot = out_b.shape[1]

    loads = [
        pltpu.make_async_copy(src, dst, load_sem.at[i])
        for i, (src, dst) in enumerate((
            (lists_hbm.at[0], lists_in.at[band]), (lat_hbm, lat_ref), (counts_hbm, counts_ref),
            (senders_hbm, senders_ref), (receivers_hbm, receivers_ref),
            (edge_hbm, state), (ew1_hbm.at[0], w1), (eb_hbm, eb_ref),
            (ew2_hbm.at[0], w2), (nw1_hbm.at[0], v1), (nw2_hbm.at[0], v2),
            (eg_hbm, eg_ref), (eo_hbm, eo_ref), (nb_hbm, nb_ref), (ng_hbm, ng_ref), (no_hbm, no_ref),
            (ew1_hbm.at[1], x1), (ew2_hbm.at[1], w2_out),
            (nw1_hbm.at[1], v1_out), (nw2_hbm.at[1], v2_out),
        ))
    ]
    for load in loads:
        load.start()

    barrier = pltpu.get_barrier_semaphore()
    for i in range(1, bands):
        pl.semaphore_signal(barrier, inc=1, device_id=(patch, lax.rem(band + i, bands)), device_id_type=MESH)

    for i in range(1, patches):
        other = lax.rem(patch + i, patches)
        for j in range(bands):
            pl.semaphore_signal(barrier, inc=1, device_id=(other, j), device_id_type=MESH)
    loads[0].wait()
    loads[1].wait()
    for c in range(bands):
        rows = lat_ref[c * nodes : (c + 1) * nodes, :]
        low_out[c] = rows.astype(BF16)
    low_in[band] = low_out[band]

    def pick_band(i):
        owner = lax.rem(band + i, bands)
        hot = lists_hot(lists_in[owner], nodes)
        if i == 0:
            own_lists[...] = hot
        out_a[i] = dot(hot, low_out[owner]).reshape(shards, slot, half).astype(BF16)
        in_a[band, patch * bands + owner] = out_a[i, me]

    pick_band(0)
    pl.semaphore_wait(barrier, shards - 1)

    def exchange(source, target, ss, rs):
        return [
            pltpu.make_async_remote_copy(
                src_ref=source(lax.rem(band + i, bands)), dst_ref=target, send_sem=ss.at[i], recv_sem=rs.at[i],
                device_id=(patch, lax.rem(band + i, bands)), device_id_type=MESH,
            )
            for i in range(1, bands)
        ]

    list_copies = exchange(lambda other: lists_in.at[band], lists_in.at[band], list_send, list_recv)
    low_copies = exchange(lambda other: low_out.at[other], low_in.at[band], low_send, low_recv)
    rest_copies = exchange(lambda other: rest_out.at[other], rest_in.at[band], rest_send, rest_recv)
    for copy in list_copies:
        copy.start()

    def to_band(shift, source, target, ss, rs):
        other = lax.rem(band + shift, bands)

        def go(k, c):
            p = lax.rem(patch + k, patches)
            pltpu.make_async_remote_copy(
                src_ref=source.at[p * bands + other], dst_ref=target, send_sem=ss, recv_sem=rs,
                device_id=(p, other), device_id_type=MESH,
            ).start()
            return c

        lax.fori_loop(0 if shift else 1, patches, go, 0)

    def to_all(source, target, ss, rs):
        def go(k, c):
            q = lax.rem(me + k, shards)
            pltpu.make_async_remote_copy(
                src_ref=source.at[q], dst_ref=target, send_sem=ss, recv_sem=rs,
                device_id=(lax.div(q, bands), lax.rem(q, bands)), device_id_type=MESH,
            ).start()
            return c

        lax.fori_loop(1, shards, go, 0)

    def from_all(source, target, ss, rs):
        others = pl.ds(0, shards - 1)
        pltpu.make_async_remote_copy(
            src_ref=source.at[others], dst_ref=target.at[others], send_sem=ss, recv_sem=rs,
            device_id=(patch, lax.rem(band + 1, bands)), device_id_type=MESH,
        ).wait()

    def send_band(i, shift):
        sender = patch * bands + lax.rem(band + i, bands)
        to_band(shift, out_a.at[i], in_a.at[band, sender], send_a.at[i], recv_a.at[i])

    for copy in low_copies:
        copy.start()
    send_band(0, 0)

    def part(c):
        return slice(c * chunk, (c + 1) * chunk)

    for load in loads[2:8]:
        load.wait()

    def matrix_of(ref):
        rows = [ref[pl.ds(j * LANES, LANES)].reshape(1, LANES) for j in range(blocks)]
        return jnp.concatenate(rows + [jnp.zeros((LANES - blocks, LANES), jnp.int32)], axis=0)

    senders, receivers = matrix_of(senders_ref).T, matrix_of(receivers_ref).T
    local_pair = pair_of(jnp.where(senders < nodes, senders, -1))
    halo_pair = pair_of(senders - nodes)
    receiver_pair = pair_of(receivers + nodes)
    lane = lax.broadcasted_iota(jnp.int32, (LANES, LANES), 1).astype(F32).astype(BF16)
    row_place = lax.broadcasted_iota(jnp.int32, (LANES, LANES), 0).astype(F32).astype(BF16)
    edge_place = lax.broadcasted_iota(jnp.int32, (1, LANES), 1)
    usable_place = lax.broadcasted_iota(jnp.int32, (LANES, LANES), 0)
    first_receiver, node_groups = nodes // LANES, 2 * nodes // LANES
    last_local = (nodes - 1) // LANES

    def build_hot(j):
        here = slice(j * LANES, (j + 1) * LANES)
        usable[here, :] = jnp.where(usable_place < counts_ref[j], 1.0, 0.0)
        local = groups_hot(*spread(local_pair, j), lane, range(last_local + 1))
        entering = groups_hot(*spread(receiver_pair, j), lane, range(first_receiver, node_groups))
        for g in range(node_groups):
            shown = [x for x in (
                local[g] if g <= last_local else None, entering[g - first_receiver] if g >= first_receiver else None
            ) if x is not None]
            node_hot[here, g * LANES : (g + 1) * LANES] = sum(shown[1:], shown[0])
        beyond = groups_hot(*spread(halo_pair, j), lane, range(halo_hot.shape[1] // LANES))
        halo_hot[here, :] = jnp.concatenate(beyond, axis=1)
        row = jnp.where(edge_place < counts_ref[j], receivers_ref[pl.ds(j * LANES, LANES)].reshape(1, LANES), -1)
        low_row, high_row = [jnp.broadcast_to(x, (LANES, LANES)) for x in pair_of(row)]
        for g, hot in enumerate(groups_hot(low_row, high_row, row_place, range(last_local + 1))):
            rows = min(LANES, nodes - g * LANES)
            scatter_hot[g * LANES : g * LANES + rows, here] = hot[0:rows]

    def own_edges(c):
        pre[part(c), :] = dot(state[part(c), :].astype(BF16), w1[0:width, :]) + eb_ref[0:1, :]
        for j in range(c * chunk // LANES, (c + 1) * chunk // LANES):
            build_hot(j)

    for c in range(chunks // 2):
        own_edges(c)
    for i in range(1, bands):
        list_copies[i - 1].wait()
        pick_band(i)
        send_band(i, 0)
    for c in range(chunks // 2, chunks):
        own_edges(c)
    for shift in range(1, bands):
        for i in range(bands):
            send_band(i, shift)
    for load in loads[8:]:
        load.wait()

    def node_products(shift):
        which = lax.rem(band + shift, bands)
        columns = low_in[which]

        def rows(first):
            return pl.ds(pl.multiple_of(first + which * half, half), half)

        return [
            dot(columns, weight[rows(first), :]) for weight, first in ((w1, width), (w1, 2 * width), (v1, 0))
        ]

    own = node_products(0)
    partial[0:nodes, :] = own[0]
    partial[nodes:, :] = own[1]
    node_pre[...] = own[2] + nb_ref[0:1, :]
    for c in range(bands):
        rest_out[c] = (lat_ref[c * nodes : (c + 1) * nodes, :] - low_out[c].astype(F32)).astype(BF16)
    rest_in[band] = rest_out[band]
    for copy in low_copies:
        copy.wait_send()
    for copy in low_copies:
        copy.wait_recv()
    for copy in rest_copies:
        copy.start()
    others = [node_products(shift) for shift in range(1, bands)]
    table[0:nodes, :] = sum([x[0] for x in others], partial[0:nodes, :]).astype(BF16)
    table[nodes:, :] = sum([x[1] for x in others], partial[nodes:, :]).astype(BF16)
    node_pre[...] = 0.5 * sum([x[2] for x in others], node_pre[...])
    for c in range(chunks):
        pre[part(c), :] = 0.5 * (pre[part(c), :] + dot(node_hot[part(c), :], table[...]))
        state[part(c), :] = with_offset(state[part(c), :], usable[part(c), :], eo_ref[0:1, :])
    for i in range(bands):
        from_all(out_a.at[i], in_a.at[0], send_a.at[i], recv_a.at[i])

    def flat(values):
        return values.astype(F32).reshape(shards * slot, values.shape[2]).astype(BF16)

    halo = jnp.concatenate([flat(in_a[i]) for i in range(bands)], axis=1)
    table_out[...] = (0.5 * dot(halo, w1[width : 2 * width, :])).astype(BF16)

    def keep(here, fresh):
        state[here, :] = fresh

    finish(
        chunks, chunk, usable, pre, halo_hot, table_out[...], w2[...], eg_ref[0:1, :],
        state, low, lambda c: c * chunk, scatter_hot, hidden, summed, keep,
    )
    for copy in rest_copies:
        copy.wait()
    wide = [low_in[i].astype(F32) + rest_in[i].astype(F32) for i in range(bands)]
    node_state = jnp.concatenate(wide, axis=1) + node_step(
        node_pre[...], summed[...], v1[width:, :], v2[...], ng_ref[0:1, :], no_ref[0:1, :]
    )
    node_out[...] = node_state
    node_low = node_state.astype(BF16)
    out_b[...] = dot(own_lists[...], node_low).reshape(shards, slot, width).astype(BF16)
    in_b[me] = out_b[me]
    to_all(out_b, in_b.at[me], send_b, recv_b)
    table[0:nodes, :] = dot(node_low, x1[width : 2 * width, :]).astype(BF16)
    table[nodes:, :] = dot(node_low, x1[2 * width :, :]).astype(BF16)
    node_pre[...] = 0.5 * (dot(node_low, v1_out[0:width, :]) + nb_ref[1:2, :])
    known_weight = jnp.concatenate([x1[0:width, :], table[...]], axis=0)
    for c in range(chunks):
        known = jnp.concatenate([low[part(c), :], node_hot[part(c), :]], axis=1)
        pre[part(c), :] = 0.5 * (dot(known, known_weight) + eb_ref[1:2, :])
        state[part(c), :] = with_offset(state[part(c), :], usable[part(c), :], eo_ref[1:2, :])
    from_all(out_b, in_b, send_b, recv_b)
    table_out[...] = (0.5 * dot(flat(in_b[...]), x1[width : 2 * width, :])).astype(BF16)


def second_kernel(
    chunk,
    state, pre, usable, halo_hot, scatter_hot, table_ref, node_ref, node_pre, w2, v1, v2,
    eg_ref, ng_ref, no_ref,
    nodes_hbm, edges_hbm,
    nodes_out, edges_out, low, hidden, summed, store_sem,
):
    edges, width = state.shape
    chunks = edges // chunk
    stores = []

    def keep(here, fresh):
        edges_out[here, :] = fresh
        store = pltpu.make_async_copy(
            edges_out.at[here], edges_hbm.at[here], store_sem.at[len(stores)]
        )
        store.start()
        stores.append(store)

    finish(
        chunks, chunk, usable, pre, halo_hot, table_ref[...], w2[...], eg_ref[1:2, :],
        state, low, lambda c: c % 2 * chunk, scatter_hot, hidden, summed, keep,
    )
    nodes_out[...] = node_ref[...] + node_step(
        node_pre[...], summed[...], v1[width:, :], v2[...], ng_ref[1:2, :], no_ref[1:2, :]
    )
    last = pltpu.make_async_copy(nodes_out, nodes_hbm, store_sem.at[chunks])
    last.start()
    for store in stores + [last]:
        store.wait()


def shards_body(
    patches, bands,
    latents, edge_latents, edge_sender, edge_receiver, block_counts, send_rows,
    edge_first_weight, edge_first_bias, edge_second_weight, edge_gain, edge_offset,
    node_first_weight, node_first_bias, node_second_weight, node_gain, node_offset,
):
    shards = patches * bands
    edges, width = edge_latents.shape
    nodes = latents.shape[0] // bands
    slot = send_rows.shape[2]
    half = latents.shape[1]
    chunk = next(c for c in (512, 256, 128) if edges % c == 0)
    far = pl.BlockSpec(memory_space=pltpu.HBM)
    near = pl.BlockSpec(memory_space=pltpu.VMEM)
    dma = pltpu.SemaphoreType.DMA

    def shaped(*shape, kind=BF16):
        return jax.ShapeDtypeStruct(shape, kind)

    def held(*shape, kind=BF16):
        return pltpu.VMEM(shape, kind)

    def afar(array):
        return pltpu.with_memory_space_constraint(array, pltpu.HBM)

    handed = pl.pallas_call(
        functools.partial(first_kernel, patches, bands, chunk),
        out_shape=(
            held(edges, width, kind=F32),
            held(edges, width, kind=F32),
            held(edges, LANES, kind=F32),
            held(edges, shards * slot),
            held(nodes, edges),
            held(shards * slot, width),
            held(nodes, width, kind=F32),
            held(nodes, width, kind=F32),
            held(*edge_second_weight.shape[1:]),
            held(*node_first_weight.shape[1:]),
            held(*node_second_weight.shape[1:]),
        ),
        in_specs=[far] * 16,
        out_specs=(near,) * 11,
        scratch_shapes=[
            pltpu.SMEM(block_counts.shape, jnp.int32),
            pltpu.VMEM(latents.shape, F32),
            pltpu.VMEM((edges,), jnp.int32),
            pltpu.VMEM((edges,), jnp.int32),
            pltpu.VMEM((bands, slot, shards), jnp.int32),
        ] + [pltpu.VMEM(edge_gain.shape, F32)] * 6 + [
            pltpu.VMEM(edge_first_weight.shape[1:], BF16),
            pltpu.VMEM(edge_second_weight.shape[1:], BF16),
            pltpu.VMEM(node_first_weight.shape[1:], BF16),
            pltpu.VMEM(node_second_weight.shape[1:], BF16),
            pltpu.VMEM(edge_first_weight.shape[1:], BF16),
            pltpu.VMEM((shards * slot, nodes), BF16),
            pltpu.VMEM((edges, 2 * nodes), BF16),
            pltpu.VMEM((2 * nodes, width), BF16),
            pltpu.VMEM((2 * nodes, width), F32),
            pltpu.VMEM((edges, width), BF16),
            pltpu.VMEM((2, chunk, width), BF16),
        ] + [pltpu.VMEM((bands, nodes, half), BF16)] * 4 + [
            pltpu.VMEM((bands, shards, slot, half), BF16),
            pltpu.VMEM((bands, shards, slot, half), BF16),
            pltpu.VMEM((shards, slot, width), BF16),
            pltpu.VMEM((shards, slot, width), BF16),
            pltpu.VMEM((nodes, width), F32),
            dma((20,)),
            dma((bands,)), dma((bands,)), dma((bands,)), dma((bands,)), dma((bands,)), dma((bands,)),
            dma((bands,)), dma((bands,)), dma, dma,
        ],
        compiler_params=pltpu.CompilerParams(
            collective_id=0, has_side_effects=True, vmem_limit_bytes=36 * 2**20
        ),
        name="layer_one",
    )(
        *map(afar, (
            block_counts, latents, edge_sender, edge_receiver, send_rows.transpose(0, 2, 1),
            edge_first_bias, edge_gain, edge_offset, node_first_bias, node_gain, node_offset,
            edge_latents, edge_first_weight, edge_second_weight, node_first_weight, node_second_weight,
        )),
    )
    return pl.pallas_call(
        functools.partial(second_kernel, chunk),
        out_shape=(shaped(nodes, width, kind=F32), shaped(edges, width, kind=F32)),
        in_specs=[near] * 14,
        out_specs=(far, far),
        scratch_shapes=[
            pltpu.VMEM((nodes, width), F32),
            pltpu.VMEM((edges, width), F32),
            pltpu.VMEM((2 * chunk, width), BF16),
            pltpu.VMEM((2, chunk, width), BF16),
            pltpu.VMEM((nodes, width), F32),
            dma((edges // chunk + 1,)),
        ],
        compiler_params=pltpu.CompilerParams(vmem_limit_bytes=24 * 2**20),
        name="layer_two",
    )(*handed, edge_gain, node_gain, node_offset)


def solution(mesh):
    owned = P(("patch", "band"))
    return jax.shard_map(
        functools.partial(shards_body, mesh.shape["patch"], mesh.shape["band"]),
        mesh=mesh,
        in_specs=(P("patch", "band"), owned, owned, owned, owned, owned) + (P(),) * 10,
        out_specs=(owned, owned),
        check_vma=False,
    )
```

```python
import functools

import jax
import jax.numpy as jnp
from jax import lax
from jax.experimental import pallas as pl
from jax.experimental.pallas import tpu as pltpu
from jax.sharding import PartitionSpec as P

epsilon = 1e-05
MESH = pl.DeviceIdType.MESH
F32 = jnp.float32
BF16 = jnp.bfloat16
LANES = 128


def dot(a, b):
    return jnp.dot(a, b, preferred_element_type=F32)


def centred(values):
    return values - jnp.mean(values, axis=-1, keepdims=True)


def inverse_spread(centre):
    return lax.rsqrt(jnp.mean(centre * centre, axis=-1, keepdims=True) + epsilon)


def swish(h):
    return (h * jnp.tanh(h) + h).astype(BF16)


def pair_of(index):
    low, high = jnp.bitwise_and(index, LANES - 1), jnp.right_shift(index, 7)
    return low.astype(F32).astype(BF16), high.astype(F32).astype(BF16)


def spread(pair, column):
    return [jnp.broadcast_to(part[:, column : column + 1], (LANES, LANES)) for part in pair]


def groups_hot(low, high, places, groups):
    one, none = jnp.ones(places.shape, BF16), jnp.zeros(places.shape, BF16)
    base = jnp.where(low == places, one, none)
    return [jnp.where(high == jnp.full(places.shape, g, BF16), base, none) for g in groups]


def lists_hot(lists, nodes):
    slots, shards = lists.shape
    place = lax.broadcasted_iota(jnp.int32, (slots, nodes), 1)
    rows = [
        jnp.where(place == jnp.broadcast_to(lists[:, q : q + 1], (slots, nodes)), 1.0, 0.0) for q in range(shards)
    ]
    return jnp.concatenate(rows, axis=0).astype(BF16)


def finish(
    chunks, chunk, usable, pre, halo_hot, halo_table, second, gain,
    base, low, low_row, scatter_hot, hidden, summed, emit,
):
    groups = base.shape[1] // LANES

    def part(c):
        return pl.ds(c * chunk, chunk)

    def gather(c):
        hidden[c % 2] = swish(dot(halo_hot[part(c), :], halo_table) + pre[part(c), :])

    def renew(c):
        centre = centred(dot(hidden[c % 2], second))
        kept = inverse_spread(centre) * usable[part(c), :]
        fresh = base[part(c), :] + centre * jnp.concatenate([kept] * groups, axis=1) * gain
        low[pl.ds(low_row(c), chunk), :] = fresh.astype(BF16)
        emit(part(c), fresh)

    def scatter(c):
        added = dot(scatter_hot[:, part(c)], low[pl.ds(low_row(c), chunk), :])
        summed[...] = added if c == 0 else summed[...] + added

    for step in range(chunks + 2):
        if 1 <= step <= chunks:
            renew(step - 1)
        if step >= 2:
            scatter(step - 2)
        if step < chunks:
            gather(step)


def node_step(node_pre, summed, first, second, gain, offset):
    h = node_pre + 0.5 * dot(summed.astype(BF16), first)
    centre = centred(dot(swish(h), second))
    return centre * inverse_spread(centre) * gain + offset


def with_offset(state, usable, offset):
    return state + jnp.concatenate([usable] * (state.shape[1] // LANES), axis=1) * offset


def first_kernel(
    patches, bands, chunk,
    counts_hbm, lat_hbm, senders_hbm, receivers_hbm, lists_hbm, eb_hbm, eg_hbm, eo_hbm, nb_hbm, ng_hbm, no_hbm,
    edge_hbm, ew1_hbm, ew2_hbm, nw1_hbm, nw2_hbm,
    state, pre, usable, halo_hot, scatter_hot, table_out, node_out, node_pre, w2_out, v1_out, v2_out,
    counts_ref, lat_ref, senders_ref, receivers_ref, lists_in, eb_ref, eg_ref, eo_ref, nb_ref, ng_ref, no_ref,
    w1, w2, v1, v2, x1, own_lists, node_hot, table, partial, low, hidden, low_out, rest_out, low_in, rest_in,
    out_a, in_a, out_b, in_b, summed,
    load_sem, list_send, list_recv, low_send, low_recv, rest_send, rest_recv, send_a, recv_a, send_b, recv_b,
):
    shards = patches * bands
    patch, band = lax.axis_index("patch"), lax.axis_index("band")
    me = patch * bands + band
    nodes = node_out.shape[0]
    edges, width = state.shape
    half = lat_ref.shape[1]
    chunks = edges // chunk
    blocks = edges // LANES
    slot = out_b.shape[1]

    loads = [
        pltpu.make_async_copy(src, dst, load_sem.at[i])
        for i, (src, dst) in enumerate((
            (lists_hbm.at[0], lists_in.at[band]), (lat_hbm, lat_ref), (counts_hbm, counts_ref),
            (senders_hbm, senders_ref), (receivers_hbm, receivers_ref),
            (edge_hbm, state), (ew1_hbm.at[0], w1), (eb_hbm, eb_ref),
            (ew2_hbm.at[0], w2), (nw1_hbm.at[0], v1), (nw2_hbm.at[0], v2),
            (eg_hbm, eg_ref), (eo_hbm, eo_ref), (nb_hbm, nb_ref), (ng_hbm, ng_ref), (no_hbm, no_ref),
            (ew1_hbm.at[1], x1), (ew2_hbm.at[1], w2_out),
            (nw1_hbm.at[1], v1_out), (nw2_hbm.at[1], v2_out),
        ))
    ]
    for load in loads:
        load.start()

    barrier = pltpu.get_barrier_semaphore()
    for i in range(1, bands):
        pl.semaphore_signal(barrier, inc=1, device_id=(patch, lax.rem(band + i, bands)), device_id_type=MESH)

    for i in range(1, patches):
        other = lax.rem(patch + i, patches)
        for j in range(bands):
            pl.semaphore_signal(barrier, inc=1, device_id=(other, j), device_id_type=MESH)
    loads[0].wait()
    loads[1].wait()
    for c in range(bands):
        rows = lat_ref[c * nodes : (c + 1) * nodes, :]
        low_out[c] = rows.astype(BF16)
    low_in[band] = low_out[band]

    def pick_band(i):
        owner = lax.rem(band + i, bands)
        hot = lists_hot(lists_in[owner], nodes)
        if i == 0:
            own_lists[...] = hot
        out_a[i] = dot(hot, low_out[owner]).reshape(shards, slot, half).astype(BF16)
        in_a[band, patch * bands + owner] = out_a[i, me]

    pick_band(0)
    pl.semaphore_wait(barrier, shards - 1)

    def exchange(source, target, ss, rs):
        return [
            pltpu.make_async_remote_copy(
                src_ref=source(lax.rem(band + i, bands)), dst_ref=target, send_sem=ss.at[i], recv_sem=rs.at[i],
                device_id=(patch, lax.rem(band + i, bands)), device_id_type=MESH,
            )
            for i in range(1, bands)
        ]

    list_copies = exchange(lambda other: lists_in.at[band], lists_in.at[band], list_send, list_recv)
    low_copies = exchange(lambda other: low_out.at[other], low_in.at[band], low_send, low_recv)
    rest_copies = exchange(lambda other: rest_out.at[other], rest_in.at[band], rest_send, rest_recv)
    for copy in list_copies:
        copy.start()

    def to_band(shift, source, target, ss, rs):
        other = lax.rem(band + shift, bands)

        for k in range(0 if shift else 1, patches):
            p = lax.rem(patch + k, patches)
            pltpu.make_async_remote_copy(
                src_ref=source.at[p * bands + other], dst_ref=target, send_sem=ss, recv_sem=rs,
                device_id=(p, other), device_id_type=MESH,
            ).start()

    def to_all(source, target, ss, rs):
        for k in range(patches):
            p = lax.rem(patch + k, patches)
            for shift in range(0 if k else 1, bands):
                other = lax.rem(band + shift, bands)
                pltpu.make_async_remote_copy(
                    src_ref=source.at[p * bands + other], dst_ref=target, send_sem=ss, recv_sem=rs,
                    device_id=(p, other), device_id_type=MESH,
                ).start()

    def from_all(source, target, ss, rs):
        others = pl.ds(0, shards - 1)
        pltpu.make_async_remote_copy(
            src_ref=source.at[others], dst_ref=target.at[others], send_sem=ss, recv_sem=rs,
            device_id=(patch, lax.rem(band + 1, bands)), device_id_type=MESH,
        ).wait()

    def send_band(i, shift):
        sender = patch * bands + lax.rem(band + i, bands)
        to_band(shift, out_a.at[i], in_a.at[band, sender], send_a.at[i], recv_a.at[i])

    for copy in low_copies:
        copy.start()
    send_band(0, 0)

    def part(c):
        return slice(c * chunk, (c + 1) * chunk)

    for load in loads[2:8]:
        load.wait()

    def matrix_of(ref):
        rows = [ref[pl.ds(j * LANES, LANES)].reshape(1, LANES) for j in range(blocks)]
        return jnp.concatenate(rows + [jnp.zeros((LANES - blocks, LANES), jnp.int32)], axis=0)

    senders, receivers = matrix_of(senders_ref).T, matrix_of(receivers_ref).T
    local_pair = pair_of(jnp.where(senders < nodes, senders, -1))
    halo_pair = pair_of(senders - nodes)
    receiver_pair = pair_of(receivers + nodes)
    lane = lax.broadcasted_iota(jnp.int32, (LANES, LANES), 1).astype(F32).astype(BF16)
    row_place = lax.broadcasted_iota(jnp.int32, (LANES, LANES), 0).astype(F32).astype(BF16)
    edge_place = lax.broadcasted_iota(jnp.int32, (1, LANES), 1)
    usable_place = lax.broadcasted_iota(jnp.int32, (LANES, LANES), 0)
    first_receiver, node_groups = nodes // LANES, 2 * nodes // LANES
    last_local = (nodes - 1) // LANES

    def build_hot(j):
        here = slice(j * LANES, (j + 1) * LANES)
        usable[here, :] = jnp.where(usable_place < counts_ref[j], 1.0, 0.0)
        local = groups_hot(*spread(local_pair, j), lane, range(last_local + 1))
        entering = groups_hot(*spread(receiver_pair, j), lane, range(first_receiver, node_groups))
        for g in range(node_groups):
            shown = [x for x in (
                local[g] if g <= last_local else None, entering[g - first_receiver] if g >= first_receiver else None
            ) if x is not None]
            node_hot[here, g * LANES : (g + 1) * LANES] = sum(shown[1:], shown[0])
        beyond = groups_hot(*spread(halo_pair, j), lane, range(halo_hot.shape[1] // LANES))
        halo_hot[here, :] = jnp.concatenate(beyond, axis=1)
        row = jnp.where(edge_place < counts_ref[j], receivers_ref[pl.ds(j * LANES, LANES)].reshape(1, LANES), -1)
        low_row, high_row = [jnp.broadcast_to(x, (LANES, LANES)) for x in pair_of(row)]
        for g, hot in enumerate(groups_hot(low_row, high_row, row_place, range(last_local + 1))):
            rows = min(LANES, nodes - g * LANES)
            scatter_hot[g * LANES : g * LANES + rows, here] = hot[0:rows]

    def own_edges(c):
        pre[part(c), :] = dot(state[part(c), :].astype(BF16), w1[0:width, :]) + eb_ref[0:1, :]
        for j in range(c * chunk // LANES, (c + 1) * chunk // LANES):
            build_hot(j)

    for c in range(chunks // 2):
        own_edges(c)
    for i in range(1, bands):
        list_copies[i - 1].wait()
        pick_band(i)
        send_band(i, 0)
    for c in range(chunks // 2, chunks):
        own_edges(c)
    for shift in range(1, bands):
        for i in range(bands):
            send_band(i, shift)
    for load in loads[8:]:
        load.wait()

    def node_products(shift):
        which = lax.rem(band + shift, bands)
        columns = low_in[which]

        def rows(first):
            return pl.ds(pl.multiple_of(first + which * half, half), half)

        return [
            dot(columns, weight[rows(first), :]) for weight, first in ((w1, width), (w1, 2 * width), (v1, 0))
        ]

    own = node_products(0)
    partial[0:nodes, :] = own[0]
    partial[nodes:, :] = own[1]
    node_pre[...] = own[2] + nb_ref[0:1, :]
    for c in range(bands):
        rest_out[c] = (lat_ref[c * nodes : (c + 1) * nodes, :] - low_out[c].astype(F32)).astype(BF16)
    rest_in[band] = rest_out[band]
    for copy in low_copies:
        copy.wait_send()
    for copy in low_copies:
        copy.wait_recv()
    for copy in rest_copies:
        copy.start()
    others = [node_products(shift) for shift in range(1, bands)]
    table[0:nodes, :] = sum([x[0] for x in others], partial[0:nodes, :]).astype(BF16)
    table[nodes:, :] = sum([x[1] for x in others], partial[nodes:, :]).astype(BF16)
    node_pre[...] = 0.5 * sum([x[2] for x in others], node_pre[...])
    for c in range(chunks):
        pre[part(c), :] = 0.5 * (pre[part(c), :] + dot(node_hot[part(c), :], table[...]))
        state[part(c), :] = with_offset(state[part(c), :], usable[part(c), :], eo_ref[0:1, :])
    for i in range(bands):
        from_all(out_a.at[i], in_a.at[0], send_a.at[i], recv_a.at[i])

    def flat(values):
        return values.astype(F32).reshape(shards * slot, values.shape[2]).astype(BF16)

    halo = jnp.concatenate([flat(in_a[i]) for i in range(bands)], axis=1)
    table_out[...] = (0.5 * dot(halo, w1[width : 2 * width, :])).astype(BF16)

    def keep(here, fresh):
        state[here, :] = fresh

    finish(
        chunks, chunk, usable, pre, halo_hot, table_out[...], w2[...], eg_ref[0:1, :],
        state, low, lambda c: c * chunk, scatter_hot, hidden, summed, keep,
    )
    for copy in rest_copies:
        copy.wait()
    wide = [low_in[i].astype(F32) + rest_in[i].astype(F32) for i in range(bands)]
    node_state = jnp.concatenate(wide, axis=1) + node_step(
        node_pre[...], summed[...], v1[width:, :], v2[...], ng_ref[0:1, :], no_ref[0:1, :]
    )
    node_out[...] = node_state
    node_low = node_state.astype(BF16)
    out_b[...] = dot(own_lists[...], node_low).reshape(shards, slot, width).astype(BF16)
    in_b[me] = out_b[me]
    to_all(out_b, in_b.at[me], send_b, recv_b)
    table[0:nodes, :] = dot(node_low, x1[width : 2 * width, :]).astype(BF16)
    table[nodes:, :] = dot(node_low, x1[2 * width :, :]).astype(BF16)
    node_pre[...] = 0.5 * (dot(node_low, v1_out[0:width, :]) + nb_ref[1:2, :])
    known_weight = jnp.concatenate([x1[0:width, :], table[...]], axis=0)
    for c in range(chunks):
        known = jnp.concatenate([low[part(c), :], node_hot[part(c), :]], axis=1)
        pre[part(c), :] = 0.5 * (dot(known, known_weight) + eb_ref[1:2, :])
        state[part(c), :] = with_offset(state[part(c), :], usable[part(c), :], eo_ref[1:2, :])
    from_all(out_b, in_b, send_b, recv_b)
    table_out[...] = (0.5 * dot(flat(in_b[...]), x1[width : 2 * width, :])).astype(BF16)


def second_kernel(
    chunk,
    state, pre, usable, halo_hot, scatter_hot, table_ref, node_ref, node_pre, w2, v1, v2,
    eg_ref, ng_ref, no_ref,
    nodes_hbm, edges_hbm,
    nodes_out, edges_out, low, hidden, summed, store_sem,
):
    edges, width = state.shape
    chunks = edges // chunk
    stores = []

    def keep(here, fresh):
        edges_out[here, :] = fresh
        store = pltpu.make_async_copy(
            edges_out.at[here], edges_hbm.at[here], store_sem.at[len(stores)]
        )
        store.start()
        stores.append(store)

    finish(
        chunks, chunk, usable, pre, halo_hot, table_ref[...], w2[...], eg_ref[1:2, :],
        state, low, lambda c: c % 2 * chunk, scatter_hot, hidden, summed, keep,
    )
    nodes_out[...] = node_ref[...] + node_step(
        node_pre[...], summed[...], v1[width:, :], v2[...], ng_ref[1:2, :], no_ref[1:2, :]
    )
    last = pltpu.make_async_copy(nodes_out, nodes_hbm, store_sem.at[chunks])
    last.start()
    for store in stores + [last]:
        store.wait()


def shards_body(
    patches, bands,
    latents, edge_latents, edge_sender, edge_receiver, block_counts, send_rows,
    edge_first_weight, edge_first_bias, edge_second_weight, edge_gain, edge_offset,
    node_first_weight, node_first_bias, node_second_weight, node_gain, node_offset,
):
    shards = patches * bands
    edges, width = edge_latents.shape
    nodes = latents.shape[0] // bands
    slot = send_rows.shape[2]
    half = latents.shape[1]
    chunk = next(c for c in (512, 256, 128) if edges % c == 0)
    far = pl.BlockSpec(memory_space=pltpu.HBM)
    near = pl.BlockSpec(memory_space=pltpu.VMEM)
    dma = pltpu.SemaphoreType.DMA

    def shaped(*shape, kind=BF16):
        return jax.ShapeDtypeStruct(shape, kind)

    def held(*shape, kind=BF16):
        return pltpu.VMEM(shape, kind)

    def afar(array):
        return pltpu.with_memory_space_constraint(array, pltpu.HBM)

    handed = pl.pallas_call(
        functools.partial(first_kernel, patches, bands, chunk),
        out_shape=(
            held(edges, width, kind=F32),
            held(edges, width, kind=F32),
            held(edges, LANES, kind=F32),
            held(edges, shards * slot),
            held(nodes, edges),
            held(shards * slot, width),
            held(nodes, width, kind=F32),
            held(nodes, width, kind=F32),
            held(*edge_second_weight.shape[1:]),
            held(*node_first_weight.shape[1:]),
            held(*node_second_weight.shape[1:]),
        ),
        in_specs=[far] * 16,
        out_specs=(near,) * 11,
        scratch_shapes=[
            pltpu.SMEM(block_counts.shape, jnp.int32),
            pltpu.VMEM(latents.shape, F32),
            pltpu.VMEM((edges,), jnp.int32),
            pltpu.VMEM((edges,), jnp.int32),
            pltpu.VMEM((bands, slot, shards), jnp.int32),
        ] + [pltpu.VMEM(edge_gain.shape, F32)] * 6 + [
            pltpu.VMEM(edge_first_weight.shape[1:], BF16),
            pltpu.VMEM(edge_second_weight.shape[1:], BF16),
            pltpu.VMEM(node_first_weight.shape[1:], BF16),
            pltpu.VMEM(node_second_weight.shape[1:], BF16),
            pltpu.VMEM(edge_first_weight.shape[1:], BF16),
            pltpu.VMEM((shards * slot, nodes), BF16),
            pltpu.VMEM((edges, 2 * nodes), BF16),
            pltpu.VMEM((2 * nodes, width), BF16),
            pltpu.VMEM((2 * nodes, width), F32),
            pltpu.VMEM((edges, width), BF16),
            pltpu.VMEM((2, chunk, width), BF16),
        ] + [pltpu.VMEM((bands, nodes, half), BF16)] * 4 + [
            pltpu.VMEM((bands, shards, slot, half), BF16),
            pltpu.VMEM((bands, shards, slot, half), BF16),
            pltpu.VMEM((shards, slot, width), BF16),
            pltpu.VMEM((shards, slot, width), BF16),
            pltpu.VMEM((nodes, width), F32),
            dma((20,)),
            dma((bands,)), dma((bands,)), dma((bands,)), dma((bands,)), dma((bands,)), dma((bands,)),
            dma((bands,)), dma((bands,)), dma, dma,
        ],
        compiler_params=pltpu.CompilerParams(
            collective_id=0, has_side_effects=True, vmem_limit_bytes=36 * 2**20
        ),
        name="layer_one",
    )(
        *map(afar, (
            block_counts, latents, edge_sender, edge_receiver, send_rows.transpose(0, 2, 1),
            edge_first_bias, edge_gain, edge_offset, node_first_bias, node_gain, node_offset,
            edge_latents, edge_first_weight, edge_second_weight, node_first_weight, node_second_weight,
        )),
    )
    return pl.pallas_call(
        functools.partial(second_kernel, chunk),
        out_shape=(shaped(nodes, width, kind=F32), shaped(edges, width, kind=F32)),
        in_specs=[near] * 14,
        out_specs=(far, far),
        scratch_shapes=[
            pltpu.VMEM((nodes, width), F32),
            pltpu.VMEM((edges, width), F32),
            pltpu.VMEM((2 * chunk, width), BF16),
            pltpu.VMEM((2, chunk, width), BF16),
            pltpu.VMEM((nodes, width), F32),
            dma((edges // chunk + 1,)),
        ],
        compiler_params=pltpu.CompilerParams(vmem_limit_bytes=24 * 2**20),
        name="layer_two",
    )(*handed, edge_gain, node_gain, node_offset)


def solution(mesh):
    owned = P(("patch", "band"))
    return jax.shard_map(
        functools.partial(shards_body, mesh.shape["patch"], mesh.shape["band"]),
        mesh=mesh,
        in_specs=(P("patch", "band"), owned, owned, owned, owned, owned) + (P(),) * 10,
        out_specs=(owned, owned),
        check_vma=False,
    )
```
